32 devices in a mesh: owner: 16 (over z, y, x), rows: 2 (over core).
Axes of the slice: x: 2, y: 2, z: 4, core: 2. Of those that a mesh axis runs over, the one named last changes fastest.
Arguments:
- train_down: float32 [64, 1024, 2048], P('owner', None, 'rows'), may hold values from -0.1875 to 0.1875
- router_weight: float32 [2048, 64], P('rows', 'owner'), may hold values from -0.125 to 0.125
- router_gain: float32 [2048], P('rows'), may hold values from 0.25 to 1.75
Outputs:
- ready_down: bfloat16 [64, 2048, 1024], P('owner')
- serve_router: bfloat16 [2048, 64], replicated
The draws below stay inside these ranges and needn't reach their ends.
All inputs are finite; a program needn't handle non-finite values.
Results may differ from the reference program's by a relative error of at most 0.001.
Values may be sent and summed in bfloat16 or wider, within the bound.
A program may use at most 128 MiB of HBM per device.

```python
import jax
import jax.numpy as jnp

EXPERTS = 64
D_MODEL = 2048
D_EXPERT = 1024


def block_levels(key, extent, shards, least, top_value):
    factor_of = 1.0
    for dim, blocks in shards:
        steps = jax.random.uniform(jax.random.fold_in(jax.random.fold_in(key, 6), dim), (blocks,), jnp.float32, least / len(shards), top_value / len(shards))
        factor_of = factor_of * jnp.repeat(jnp.exp(steps), extent[dim] // blocks).reshape((-1,) + (1,) * (len(extent) - 1 - dim))
    return factor_of


def noise(stream_key, shape, spread, most, split=(), dtype=jnp.bfloat16):
    factor_of = block_levels(stream_key, shape, split, -0.22, 0.18) if split else 1.0
    values = jax.random.normal(stream_key, shape, jnp.float32) * spread * factor_of
    return jnp.minimum(jnp.maximum(values, -most), most).astype(dtype)


def setup_inputs(seed: int = 0) -> dict:
    streams_of = jax.random.split(jax.random.key(seed), 4)
    return {
        "train_down": noise(streams_of[0], (EXPERTS, D_EXPERT, D_MODEL), D_EXPERT ** -0.5, 0.1875, ((0, 16), (2, 2)), jnp.float32),
        "router_weight": noise(streams_of[1], (D_MODEL, EXPERTS), D_MODEL ** -0.5, 0.125, ((0, 2), (1, 16)), jnp.float32),
        "router_gain": jnp.clip(1.0 + 0.15 * jax.random.normal(streams_of[2], (D_MODEL,), jnp.float32), 0.25, 1.75),
    }


def reference(train_down, router_weight, router_gain):
    ready_down = train_down.astype(jnp.bfloat16)
    ready_down = jnp.transpose(ready_down, (0, 2, 1))
    serve_router = (router_weight * router_gain[:, None]).astype(jnp.bfloat16)
    return ready_down, serve_router
```

```python
import functools

import jax
import jax.numpy as jnp
from jax import lax
from jax.experimental import pallas as pl
from jax.experimental.pallas import tpu as pltpu
from jax.sharding import PartitionSpec as P

MESH = pl.DeviceIdType.MESH
AHEAD = 6


def exchange_kernel(
    owners, rows, tile,
    down, weight, gain, ready, router,
    landed, load_sem, send_sem, recv_sem,
    row_send, row_recv, own_send, own_recv,
):
    owner, row = lax.axis_index("owner"), lax.axis_index("rows")
    experts, _, width = down.shape
    part = weight.shape[1]
    per = width // tile
    steps = experts * per

    def load(i):
        source = down.at[i // per, :, pl.ds(pl.multiple_of((i % per) * tile, tile), tile)]
        return pltpu.make_async_copy(source, landed.at[i], load_sem.at[i])

    def place(i, r):
        start = pl.multiple_of(r * width + (i % per) * tile, tile)
        return ready.at[i // per, pl.ds(start, tile), :]

    def send(i, j):
        return pltpu.make_async_remote_copy(
            src_ref=place(i, row), dst_ref=place(i, row),
            send_sem=send_sem.at[j - 1, i], recv_sem=recv_sem.at[j - 1, i],
            device_id=(owner, lax.rem(row + j, rows)), device_id_type=MESH,
        )

    def row_place(r):
        return router.at[owner, :, pl.ds(pl.multiple_of(r * part, part), part)]

    def row_copy(j):
        return pltpu.make_async_remote_copy(
            src_ref=row_place(row), dst_ref=row_place(row),
            send_sem=row_send.at[j - 1], recv_sem=row_recv.at[j - 1],
            device_id=(owner, lax.rem(row + j, rows)), device_id_type=MESH,
        )

    def own_copy(j):
        return pltpu.make_async_remote_copy(
            src_ref=router.at[owner], dst_ref=router.at[owner],
            send_sem=own_send.at[j - 1], recv_sem=own_recv.at[j - 1],
            device_id=(lax.rem(owner + j, owners), row), device_id_type=MESH,
        )

    ahead = min(AHEAD, steps)
    for i in range(ahead):
        load(i).start()

    barrier = pltpu.get_barrier_semaphore()
    for j in range(1, rows):
        pl.semaphore_signal(
            barrier, inc=1, device_id=(owner, lax.rem(row + j, rows)), device_id_type=MESH)

    @pl.loop(1, owners)
    def _(j):
        pl.semaphore_signal(
            barrier, inc=1, device_id=(lax.rem(owner + j, owners), row), device_id_type=MESH)

    router[owner, :, pl.ds(pl.multiple_of(row * part, part), part)] = (
        weight[...] * gain[...]).astype(jnp.bfloat16)

    def turn(i):
        load(i).wait()
        start = pl.multiple_of(row * width + (i % per) * tile, tile)
        ready[i // per, pl.ds(start, tile), :] = landed[i].T.astype(jnp.bfloat16)

        @pl.when(i + ahead < steps)
        def _():
            load(i + ahead).start()

    turn(0)
    pl.semaphore_wait(barrier, rows - 1 + owners - 1)
    for j in range(1, rows):
        row_copy(j).start()
        send(0, j).start()

    if steps > 1:
        @pl.loop(1, steps)
        def _(i):
            turn(i)
            for j in range(1, rows):
                send(i, j).start()

    for j in range(1, rows):
        row_copy(j).wait()

    @pl.loop(1, owners)
    def _(j):
        own_copy(j).start()

    @pl.loop(1, owners)
    def _(j):
        own_copy(j).wait()

    @pl.loop(0, steps)
    def _(i):
        for j in range(1, rows):
            send(i, j).wait()


def write_kernel(pieces, ready, out, sems):
    size = ready.shape[0] // pieces

    def copy(i):
        span = pl.ds(i * size, size)
        return pltpu.make_async_copy(ready.at[span], out.at[span], sems.at[i])

    for i in range(pieces):
        copy(i).start()
    for i in range(pieces):
        copy(i).wait()


def on_device(owners, rows, train_down, router_weight, router_gain):
    experts, depth, width = train_down.shape
    part, local = router_weight.shape
    tile = min(256, width)
    steps = experts * (width // tile)
    vmem = pl.BlockSpec(memory_space=pltpu.VMEM)
    anywhere = pl.BlockSpec(memory_space=pl.ANY)
    full = rows * width
    ready, router = pl.pallas_call(
        functools.partial(exchange_kernel, owners, rows, tile),
        out_shape=(
            pltpu.VMEM((experts, full, depth), jnp.bfloat16),
            pltpu.VMEM((owners, local, rows * part), jnp.bfloat16),
        ),
        in_specs=[anywhere, vmem, vmem],
        out_specs=(vmem, vmem),
        scratch_shapes=[
            pltpu.VMEM((steps, depth, tile), jnp.float32),
            pltpu.SemaphoreType.DMA((steps,)),
            pltpu.SemaphoreType.DMA((rows - 1, steps)),
            pltpu.SemaphoreType.DMA((rows - 1, steps)),
            pltpu.SemaphoreType.DMA((rows - 1,)),
            pltpu.SemaphoreType.DMA((rows - 1,)),
            pltpu.SemaphoreType.DMA((owners - 1,)),
            pltpu.SemaphoreType.DMA((owners - 1,)),
        ],
        compiler_params=pltpu.CompilerParams(
            collective_id=0, has_side_effects=True, vmem_limit_bytes=22 * 2**20),
        name="exchange",
    )(train_down, router_weight.T, router_gain.reshape(1, part))
    flat = ready.reshape(experts * full, depth)
    pieces = 8
    out = pl.pallas_call(
        functools.partial(write_kernel, pieces),
        out_shape=jax.ShapeDtypeStruct((experts * full, depth), jnp.bfloat16),
        in_specs=[vmem],
        out_specs=anywhere,
        scratch_shapes=[pltpu.SemaphoreType.DMA((pieces,))],
        compiler_params=pltpu.CompilerParams(vmem_limit_bytes=4 * 2**20),
        name="write",
    )(flat)
    serve = router.reshape(owners * local, rows * part).T
    return out.reshape(experts, full, depth), serve


def solution(mesh):
    owners, rows = mesh.shape["owner"], mesh.shape["rows"]
    return jax.shard_map(
        functools.partial(on_device, owners, rows),
        mesh=mesh,
        in_specs=(P("owner", None, "rows"), P("rows", "owner"), P("rows")),
        out_specs=(P("owner", None, None), P()),
        check_vma=False,
    )
```

```python
import functools

import jax
import jax.numpy as jnp
from jax import lax
from jax.experimental import pallas as pl
from jax.experimental.pallas import tpu as pltpu
from jax.sharding import PartitionSpec as P

MESH = pl.DeviceIdType.MESH
AHEAD = 6


def exchange_kernel(
    owners, rows, tile,
    down, weight, gain, ready, router,
    landed, weight_here, gain_here, load_sem, small_sem, send_sem, recv_sem,
    row_send, row_recv, own_send, own_recv, near, go, all_in,
):
    owner, row = lax.axis_index("owner"), lax.axis_index("rows")
    experts, _, width = down.shape
    part = weight.shape[1]
    per = width // tile
    steps = experts * per

    def load(i):
        source = down.at[i // per, :, pl.ds(pl.multiple_of((i % per) * tile, tile), tile)]
        return pltpu.make_async_copy(source, landed.at[i], load_sem.at[i])

    def place(i):
        start = pl.multiple_of(row * width + (i % per) * tile, tile)
        return ready.at[i // per, pl.ds(start, tile), :]

    def send(i, j):
        return pltpu.make_async_remote_copy(
            src_ref=place(i), dst_ref=place(i),
            send_sem=send_sem.at[j - 1, i], recv_sem=recv_sem.at[j - 1, i],
            device_id=(owner, lax.rem(row + j, rows)), device_id_type=MESH,
        )

    def row_copy(j):
        mine = router.at[owner, :, pl.ds(pl.multiple_of(row * part, part), part)]
        return pltpu.make_async_remote_copy(
            src_ref=mine, dst_ref=mine,
            send_sem=row_send.at[j - 1], recv_sem=row_recv.at[j - 1],
            device_id=(owner, lax.rem(row + j, rows)), device_id_type=MESH,
        )

    def own_copy(j):
        return pltpu.make_async_remote_copy(
            src_ref=router.at[owner], dst_ref=router.at[owner],
            send_sem=own_send.at[j - 1], recv_sem=own_recv.at[j - 1],
            device_id=(lax.rem(owner + j, owners), row), device_id_type=MESH,
        )

    def signal(sem, o, r):
        pl.semaphore_signal(sem, inc=1, device_id=(o, r), device_id_type=MESH)

    barrier = pltpu.get_barrier_semaphore()

    @pl.when(row == 0)
    def _():
        for r in range(1, rows):
            signal(barrier, owner, r)

    copies = (
        pltpu.make_async_copy(weight, weight_here, small_sem.at[0]),
        pltpu.make_async_copy(gain, gain_here, small_sem.at[1]),
    )
    for copy in copies:
        copy.start()
    ahead = min(AHEAD, steps)
    for i in range(ahead):
        load(i).start()

    @pl.when(row != 0)
    def _():
        pl.semaphore_wait(barrier, 1)
        signal(near, owner, 0)

    @pl.when(row == 0)
    def _():
        pl.semaphore_wait(near, rows - 1)
        for r in range(1, rows):
            signal(go, owner, r)

        @pl.loop(1, owners)
        def _(j):
            signal(barrier, lax.rem(owner + j, owners), 0)

    for copy in copies:
        copy.wait()
    router[owner, :, pl.ds(pl.multiple_of(row * part, part), part)] = (
        weight_here[...] * gain_here[...]).astype(jnp.bfloat16)

    def turn(i):
        load(i).wait()
        start = pl.multiple_of(row * width + (i % per) * tile, tile)
        ready[i // per, pl.ds(start, tile), :] = landed[i].T.astype(jnp.bfloat16)

        @pl.when(i + ahead < steps)
        def _():
            load(i + ahead).start()

    def turn_and_send(i):
        turn(i)
        for j in range(1, rows):
            send(i, j).start()

    turn(0)

    @pl.when(row != 0)
    def _():
        pl.semaphore_wait(go, 1)

    for j in range(1, rows):
        row_copy(j).start()
        send(0, j).start()

    half = max(1, steps // 2)
    if half > 1:
        pl.loop(1, half)(turn_and_send)

    for j in range(1, rows):
        row_copy(j).wait()

    @pl.when(row == 0)
    def _():
        pl.semaphore_wait(barrier, owners - 1)
        for r in range(1, rows):
            signal(all_in, owner, r)

    @pl.when(row != 0)
    def _():
        pl.semaphore_wait(all_in, 1)

    @pl.loop(1, owners)
    def _(j):
        own_copy(j).start()

    if steps > half:
        pl.loop(half, steps)(turn_and_send)

    @pl.loop(0, steps)
    def _(i):
        for j in range(1, rows):
            send(i, j).wait()

    @pl.loop(1, owners)
    def _(j):
        own_copy(j).wait()


def write_kernel(pieces, ready, router, out, serve, sems):
    size = ready.shape[0] // pieces
    local = router.shape[1]

    def copy(i):
        span = pl.ds(i * size, size)
        return pltpu.make_async_copy(ready.at[span], out.at[span], sems.at[i])

    for i in range(pieces):
        copy(i).start()
    for o in range(router.shape[0]):
        serve[o * local:(o + 1) * local, :] = router[o]
    for i in range(pieces):
        copy(i).wait()


def on_device(owners, rows, train_down, router_weight, router_gain):
    experts, depth, width = train_down.shape
    part, local = router_weight.shape
    tile = min(256, width)
    steps = experts * (width // tile)
    vmem = pl.BlockSpec(memory_space=pltpu.VMEM)
    anywhere = pl.BlockSpec(memory_space=pl.ANY)
    full = rows * width
    ready, router = pl.pallas_call(
        functools.partial(exchange_kernel, owners, rows, tile),
        out_shape=(
            pltpu.VMEM((experts, full, depth), jnp.bfloat16),
            pltpu.VMEM((owners, local, rows * part), jnp.bfloat16),
        ),
        in_specs=[anywhere, anywhere, anywhere],
        out_specs=(vmem, vmem),
        scratch_shapes=[
            pltpu.VMEM((steps, depth, tile), jnp.float32),
            pltpu.VMEM((local, part), jnp.float32),
            pltpu.VMEM((1, part), jnp.float32),
            pltpu.SemaphoreType.DMA((steps,)),
            pltpu.SemaphoreType.DMA((2,)),
            pltpu.SemaphoreType.DMA((rows - 1, steps)),
            pltpu.SemaphoreType.DMA((rows - 1, steps)),
            pltpu.SemaphoreType.DMA((rows - 1,)),
            pltpu.SemaphoreType.DMA((rows - 1,)),
            pltpu.SemaphoreType.DMA((owners - 1,)),
            pltpu.SemaphoreType.DMA((owners - 1,)),
            pltpu.SemaphoreType.REGULAR,
            pltpu.SemaphoreType.REGULAR,
            pltpu.SemaphoreType.REGULAR,
        ],
        compiler_params=pltpu.CompilerParams(
            collective_id=0, has_side_effects=True, vmem_limit_bytes=22 * 2**20),
        name="exchange",
    )(*(
        pltpu.with_memory_space_constraint(a, pltpu.HBM)
        for a in (train_down, router_weight.T, router_gain.reshape(1, part))))
    flat = ready.reshape(experts * full, depth)
    pieces = 8
    out, serve = pl.pallas_call(
        functools.partial(write_kernel, pieces),
        out_shape=(
            jax.ShapeDtypeStruct((experts * full, depth), jnp.bfloat16),
            jax.ShapeDtypeStruct((owners * local, rows * part), jnp.bfloat16),
        ),
        in_specs=[vmem, vmem],
        out_specs=(anywhere, vmem),
        scratch_shapes=[pltpu.SemaphoreType.DMA((pieces,))],
        compiler_params=pltpu.CompilerParams(vmem_limit_bytes=4 * 2**20),
        name="write",
    )(flat, router)
    return out.reshape(experts, full, depth), serve.T


def solution(mesh):
    owners, rows = mesh.shape["owner"], mesh.shape["rows"]
    return jax.shard_map(
        functools.partial(on_device, owners, rows),
        mesh=mesh,
        in_specs=(P("owner", None, "rows"), P("rows", "owner"), P("rows")),
        out_specs=(P("owner", None, None), P()),
        check_vma=False,
    )
```

```python
import functools

import jax
import jax.numpy as jnp
from jax import lax
from jax.experimental import pallas as pl
from jax.experimental.pallas import tpu as pltpu
from jax.sharding import PartitionSpec as P

MESH = pl.DeviceIdType.MESH
AHEAD = 6
LATE = 8


def exchange_kernel(
    owners, rows, tile, late,
    down, weight, gain, ready, router, later,
    landed, weight_here, gain_here, load_sem, small_sem, send_sem, recv_sem,
    row_send, row_recv, own_send, own_recv, near, go, all_in, later_sem,
):
    owner, row = lax.axis_index("owner"), lax.axis_index("rows")
    experts, _, width = down.shape
    part = weight.shape[1]
    per = width // tile
    steps = experts * per
    early = steps - late

    def load(i):
        source = down.at[i // per, :, pl.ds(pl.multiple_of((i % per) * tile, tile), tile)]
        return pltpu.make_async_copy(source, landed.at[i], load_sem.at[i])

    def place(i):
        start = pl.multiple_of(row * width + (i % per) * tile, tile)
        return ready.at[i // per, pl.ds(start, tile), :]

    def send(i, j):
        return pltpu.make_async_remote_copy(
            src_ref=place(i), dst_ref=place(i),
            send_sem=send_sem.at[j - 1, i], recv_sem=recv_sem.at[j - 1, i],
            device_id=(owner, lax.rem(row + j, rows)), device_id_type=MESH,
        )

    def row_copy(j):
        mine = router.at[owner, :, pl.ds(pl.multiple_of(row * part, part), part)]
        return pltpu.make_async_remote_copy(
            src_ref=mine, dst_ref=mine,
            send_sem=row_send.at[j - 1], recv_sem=row_recv.at[j - 1],
            device_id=(owner, lax.rem(row + j, rows)), device_id_type=MESH,
        )

    def own_copy(j):
        return pltpu.make_async_remote_copy(
            src_ref=router.at[owner], dst_ref=router.at[owner],
            send_sem=own_send.at[j - 1], recv_sem=own_recv.at[j - 1],
            device_id=(lax.rem(owner + j, owners), row), device_id_type=MESH,
        )

    def signal(sem, o, r):
        pl.semaphore_signal(sem, inc=1, device_id=(o, r), device_id_type=MESH)

    barrier = pltpu.get_barrier_semaphore()

    @pl.when(row == 0)
    def _():
        for r in range(1, rows):
            signal(barrier, owner, r)

    copies = (
        pltpu.make_async_copy(weight, weight_here, small_sem.at[0]),
        pltpu.make_async_copy(gain, gain_here, small_sem.at[1]),
    )
    for copy in copies:
        copy.start()
    ahead = min(AHEAD, steps)
    for i in range(ahead):
        load(i).start()

    @pl.when(row != 0)
    def _():
        pl.semaphore_wait(barrier, 1)
        signal(near, owner, 0)

    @pl.when(row == 0)
    def _():
        pl.semaphore_wait(near, rows - 1)
        for r in range(1, rows):
            signal(go, owner, r)

        @pl.loop(1, owners)
        def _(j):
            signal(barrier, lax.rem(owner + j, owners), 0)

    for copy in copies:
        copy.wait()
    router[owner, :, pl.ds(pl.multiple_of(row * part, part), part)] = (
        weight_here[...] * gain_here[...]).astype(jnp.bfloat16)

    def turn(i):
        load(i).wait()
        start = pl.multiple_of(row * width + (i % per) * tile, tile)
        ready[i // per, pl.ds(start, tile), :] = landed[i].T.astype(jnp.bfloat16)

        @pl.when(i + ahead < steps)
        def _():
            load(i + ahead).start()

    def turn_and_send(i):
        turn(i)
        for j in range(1, rows):
            send(i, j).start()

    def keep(i):
        start = pl.multiple_of((i - early) * tile, tile)
        return pltpu.make_async_copy(
            place(i), later.at[pl.ds(start, tile), :], later_sem.at[i - early])

    turn(0)

    @pl.when(row != 0)
    def _():
        pl.semaphore_wait(go, 1)

    for j in range(1, rows):
        row_copy(j).start()
        send(0, j).start()

    half = max(1, early // 2)
    if half > 1:
        pl.loop(1, half)(turn_and_send)

    for j in range(1, rows):
        row_copy(j).wait()

    @pl.when(row == 0)
    def _():
        pl.semaphore_wait(barrier, owners - 1)
        for r in range(1, rows):
            signal(all_in, owner, r)

    @pl.when(row != 0)
    def _():
        pl.semaphore_wait(all_in, 1)

    @pl.loop(1, owners)
    def _(j):
        own_copy(j).start()

    if early > half:
        pl.loop(half, early)(turn_and_send)

    @pl.loop(early, steps)
    def _(i):
        turn(i)
        keep(i).start()

    @pl.loop(early, steps)
    def _(i):
        keep(i).wait()

    @pl.loop(0, early)
    def _(i):
        for j in range(1, rows):
            send(i, j).wait()

    @pl.loop(1, owners)
    def _(j):
        own_copy(j).wait()


def write_kernel(rows, width, held, ready, router, out, serve, laid, sems, last_sem, serve_sem):
    row = lax.axis_index("rows")
    experts, full, _ = ready.shape
    local = router.shape[1]
    whole = experts - 1

    def copy(e):
        return pltpu.make_async_copy(ready.at[e], out.at[e], sems.at[e])

    def last(j):
        start = pl.multiple_of(lax.rem(row + j, rows) * width, width)
        span = pl.ds(start, width if j == 0 else width - held)
        return pltpu.make_async_copy(
            ready.at[whole, span, :], out.at[whole, span, :], last_sem.at[j])

    lasts = [last(j) for j in range(rows) if j == 0 or held < width]
    for e in range(whole):
        copy(e).start()
    for part in lasts:
        part.start()
    for o in range(router.shape[0]):
        laid[o * local:(o + 1) * local, :] = router[o]
    spread = pltpu.make_async_copy(laid, serve, serve_sem)
    spread.start()
    for e in range(whole):
        copy(e).wait()
    for part in lasts:
        part.wait()
    spread.wait()


def put_kernel(rows, width, *refs):
    row = lax.axis_index("rows")
    gots, out, sems = refs[:rows - 1], refs[-2], refs[-1]
    pieces = sems.shape[1]
    held = gots[0].shape[0]
    size = held // pieces

    def copy(j, i):
        source = lax.rem(row + rows - j, rows)
        start = pl.multiple_of(source * width + (width - held) + i * size, size)
        return pltpu.make_async_copy(
            gots[j - 1].at[pl.ds(i * size, size), :],
            out.at[out.shape[0] - 1, pl.ds(start, size), :], sems.at[j - 1, i])

    for j in range(1, rows):
        for i in range(pieces):
            copy(j, i).start()
    for j in range(1, rows):
        for i in range(pieces):
            copy(j, i).wait()


def on_device(owners, rows, train_down, router_weight, router_gain):
    experts, depth, width = train_down.shape
    part, local = router_weight.shape
    tile = min(128, width)
    per = width // tile
    steps = experts * per
    late = LATE if steps > LATE and per >= LATE else 1
    held = late * tile
    vmem = pl.BlockSpec(memory_space=pltpu.VMEM)
    anywhere = pl.BlockSpec(memory_space=pl.ANY)
    full = rows * width
    ready, router, later = pl.pallas_call(
        functools.partial(exchange_kernel, owners, rows, tile, late),
        out_shape=(
            pltpu.VMEM((experts, full, depth), jnp.bfloat16),
            pltpu.VMEM((owners, local, rows * part), jnp.bfloat16),
            pltpu.HBM((held, depth), jnp.bfloat16),
        ),
        in_specs=[anywhere, anywhere, anywhere],
        out_specs=(vmem, vmem, anywhere),
        scratch_shapes=[
            pltpu.VMEM((steps, depth, tile), jnp.float32),
            pltpu.VMEM((local, part), jnp.float32),
            pltpu.VMEM((1, part), jnp.float32),
            pltpu.SemaphoreType.DMA((steps,)),
            pltpu.SemaphoreType.DMA((2,)),
            pltpu.SemaphoreType.DMA((rows - 1, steps)),
            pltpu.SemaphoreType.DMA((rows - 1, steps)),
            pltpu.SemaphoreType.DMA((rows - 1,)),
            pltpu.SemaphoreType.DMA((rows - 1,)),
            pltpu.SemaphoreType.DMA((owners - 1,)),
            pltpu.SemaphoreType.DMA((owners - 1,)),
            pltpu.SemaphoreType.REGULAR,
            pltpu.SemaphoreType.REGULAR,
            pltpu.SemaphoreType.REGULAR,
            pltpu.SemaphoreType.DMA((late,)),
        ],
        compiler_params=pltpu.CompilerParams(
            collective_id=0, has_side_effects=True, vmem_limit_bytes=22 * 2**20),
        name="exchange",
    )(*(
        pltpu.with_memory_space_constraint(a, pltpu.HBM)
        for a in (train_down, router_weight.T, router_gain.reshape(1, part))))
    got = [
        lax.ppermute(later, "rows", [(r, (r + j) % rows) for r in range(rows)])
        for j in range(1, rows)
    ]
    shape = jax.ShapeDtypeStruct((experts, full, depth), jnp.bfloat16)
    out, serve = pl.pallas_call(
        functools.partial(write_kernel, rows, width, held),
        out_shape=(
            shape,
            jax.ShapeDtypeStruct((owners * local, rows * part), jnp.bfloat16),
        ),
        in_specs=[vmem, vmem],
        out_specs=(anywhere, anywhere),
        scratch_shapes=[
            pltpu.VMEM((owners * local, rows * part), jnp.bfloat16),
            pltpu.SemaphoreType.DMA((experts,)),
            pltpu.SemaphoreType.DMA((rows,)),
            pltpu.SemaphoreType.DMA,
        ],
        compiler_params=pltpu.CompilerParams(vmem_limit_bytes=4 * 2**20),
        cost_estimate=pl.CostEstimate(
            flops=0, bytes_accessed=experts * full * depth * 4, transcendentals=0),
        name="write",
    )(ready, router)
    pieces = 2
    out = pl.pallas_call(
        functools.partial(put_kernel, rows, width),
        out_shape=shape,
        in_specs=[vmem] * (rows - 1) + [anywhere],
        out_specs=anywhere,
        input_output_aliases={rows - 1: 0},
        scratch_shapes=[pltpu.SemaphoreType.DMA((rows - 1, pieces))],
        compiler_params=pltpu.CompilerParams(vmem_limit_bytes=2 * 2**20),
        name="put",
    )(*got, out)
    return out, serve.T


def solution(mesh):
    owners, rows = mesh.shape["owner"], mesh.shape["rows"]
    return jax.shard_map(
        functools.partial(on_device, owners, rows),
        mesh=mesh,
        in_specs=(P("owner", None, "rows"), P("rows", "owner"), P("rows")),
        out_specs=(P("owner", None, None), P()),
        check_vma=False,
    )
```
